32 devices in a mesh: shard: 2 (over core), model: 4 (over y, x), unit: 4 (over z).
Axes of the slice: x: 2, y: 2, z: 4, core: 2. Of those that a mesh axis runs over, the one named last changes fastest.
Arguments:
- train_query: bfloat16 [16384, 4096], P(('unit', 'shard'), 'model'), parts along dimension 0, may hold values from -0.125 to 0.125
- low_query: bfloat16 [16384, 16], P(('unit', 'shard')), parts along dimension 0, may hold values from -0.09375 to 0.09375
- high_query: bfloat16 [64, 4096], P('unit', 'model'), parts along dimension 0, may hold values from -1.5 to 1.5
- train_key: bfloat16 [16384, 1024], P(('unit', 'shard'), 'model'), parts along dimension 0, may hold values from -0.125 to 0.125
- low_key: bfloat16 [16384, 16], P(('unit', 'shard')), parts along dimension 0, may hold values from -0.09375 to 0.09375
- high_key: bfloat16 [64, 1024], P('unit', 'model'), parts along dimension 0, may hold values from -1.5 to 1.5
- train_value: bfloat16 [16384, 1024], P(('unit', 'shard'), 'model'), parts along dimension 0, may hold values from -0.125 to 0.125
- low_value: bfloat16 [16384, 16], P(('unit', 'shard')), parts along dimension 0, may hold values from -0.09375 to 0.09375
- high_value: bfloat16 [64, 1024], P('unit', 'model'), parts along dimension 0, may hold values from -1.5 to 1.5
- norm_train: float32 [16384], P(('unit', 'shard', 'model')), parts along dimension 0, may hold values from 0.25 to 1.75
- norm_step: float32 [16384], P(('unit', 'shard', 'model')), parts along dimension 0, may hold values from -0.3 to 0.3
Outputs:
- serving_query: bfloat16 [16384, 4096], P('unit', 'model'), parts along dimension 0
- serving_key: bfloat16 [16384, 1024], P('unit', 'model'), parts along dimension 0
- serving_value: bfloat16 [16384, 1024], P('unit', 'model'), parts along dimension 0
- scale_query: float32 [16384], P(('unit', 'model')), parts along dimension 0
- scale_key: float32 [4096], P(('unit', 'model')), parts along dimension 0
- scale_value: float32 [4096], P(('unit', 'model')), parts along dimension 0
- serve_norm: bfloat16 [16384], P('unit'), parts along dimension 0
The draws below stay inside these ranges and needn't reach their ends.
There are 4 independent parts, one for each index of `unit`. The reference program is written for one: setup_inputs(seed, part) draws one part's arguments, and reference() takes and returns one part's arrays. A program takes and returns all parts, laid end to end along the dimension named above; each array names one. Nothing has to cross between parts.
All inputs are finite; a program needn't handle non-finite values. Where the reference program divides by a largest or mean magnitude, that divisor is 1e-20 or more.
Results may differ from the reference program's by a relative error of at most 0.001.
Values may be sent and summed in bfloat16 or wider, within the bound.
A program may use at most 64 MiB of HBM per device.

```python
import jax
import jax.numpy as jnp

D_MODEL = 4096
Q_DIM = 4096
KV_DIM = 1024
RANK = 16


def with_spikes(values, key, source, target, shards_of, factor):
    owner, partner = [(jnp.arange(values.shape[position]) // (values.shape[position] // shards_of)).reshape([-1 if axis == position else 1 for axis in range(values.ndim)]) for position in (source, target)]
    chosen = jax.random.permutation(key, shards_of)[partner]
    strong = (owner == chosen) | (owner == (partner + shards_of // 2) % shards_of)
    return jnp.where(strong, factor * values, values)


def block_levels(rng, extent, pieces, low, largest):
    loudness, own = 1.0, jax.random.fold_in(rng, 6)
    for dim, parts in pieces:
        steps = jnp.exp(jax.random.uniform(jax.random.fold_in(own, dim), (parts,), jnp.float32, low / len(pieces), largest / len(pieces)))
        loudness = loudness * jnp.repeat(steps, extent[dim] // parts).reshape([-1 if axis == dim else 1 for axis in range(len(extent))])
    return loudness


def bell_draw(key, dims, deviation, most, pieces=(), held_as=jnp.bfloat16):
    loudness = block_levels(key, dims, pieces, -0.22, 0.18) if pieces else 1.0
    drawn = jax.random.normal(key, dims, jnp.float32) * deviation * loudness
    return jnp.minimum(jnp.maximum(drawn, -most), most).astype(held_as)


def noise_with(rng, extent, width, most, shards, heavy, held_as=jnp.bfloat16):
    drawn = width * jax.random.normal(rng, extent, jnp.float32)
    if shards:
        drawn = drawn * block_levels(rng, extent, shards, -0.22, 0.18)
    return jnp.clip(with_spikes(drawn, jax.random.fold_in(rng, 3), *heavy), -most, most).astype(held_as)


def setup_inputs(seed: int = 0, part: int = 0) -> dict:
    key_list = jax.random.split(jax.random.key(seed), 12)
    part_splits = jax.random.split(jax.random.fold_in(key_list[11], part), 12)
    return {
        "train_query": noise_with(part_splits[0], (D_MODEL, Q_DIM), D_MODEL ** -0.5, 0.125, ((0, 2), (1, 4)), (0, 1, 4, 2.0)),
        "low_query": bell_draw(part_splits[1], (D_MODEL, RANK), D_MODEL ** -0.5, 0.09375, ((0, 2),)),
        "high_query": bell_draw(part_splits[2], (RANK, Q_DIM), RANK ** -0.5, 1.5, ((1, 4),)),
        "train_key": noise_with(part_splits[3], (D_MODEL, KV_DIM), D_MODEL ** -0.5, 0.125, ((0, 2), (1, 4)), (0, 1, 4, 2.0)),
        "low_key": bell_draw(part_splits[4], (D_MODEL, RANK), D_MODEL ** -0.5, 0.09375, ((0, 2),)),
        "high_key": bell_draw(part_splits[5], (RANK, KV_DIM), RANK ** -0.5, 1.5, ((1, 4),)),
        "train_value": noise_with(part_splits[6], (D_MODEL, KV_DIM), D_MODEL ** -0.5, 0.125, ((0, 2), (1, 4)), (0, 1, 4, 2.0)),
        "low_value": bell_draw(part_splits[7], (D_MODEL, RANK), D_MODEL ** -0.5, 0.09375, ((0, 2),)),
        "high_value": bell_draw(part_splits[8], (RANK, KV_DIM), RANK ** -0.5, 1.5, ((1, 4),)),
        "norm_train": jnp.clip(1.0 + 0.15 * jax.random.normal(part_splits[9], (D_MODEL,), jnp.float32), 0.25, 1.75),
        "norm_step": jnp.clip(jax.random.uniform(part_splits[10], (D_MODEL,), jnp.float32, -0.3, 0.3) * block_levels(part_splits[10], (D_MODEL,), ((0, 8),), -0.4, 0.0), -0.3, 0.3),
    }


mix_rate = 1.0


def reference(train_query, low_query, high_query, train_key, low_key, high_key, train_value, low_value, high_value, norm_train, norm_step):
    whole_query = train_query.astype(jnp.float32) + mix_rate * jnp.dot(low_query, high_query, preferred_element_type=jnp.float32)
    whole_key = train_key.astype(jnp.float32) + mix_rate * jnp.dot(low_key, high_key, preferred_element_type=jnp.float32)
    whole_value = train_value.astype(jnp.float32) + mix_rate * jnp.dot(low_value, high_value, preferred_element_type=jnp.float32)
    scale_query = jnp.max(jnp.abs(whole_query), axis=0)
    serving_query = (whole_query / scale_query).astype(jnp.bfloat16)
    scale_key = jnp.max(jnp.abs(whole_key), axis=0)
    serving_key = (whole_key / scale_key).astype(jnp.bfloat16)
    scale_value = jnp.max(jnp.abs(whole_value), axis=0)
    serving_value = (whole_value / scale_value).astype(jnp.bfloat16)
    serve_norm = (norm_train + norm_step).astype(jnp.bfloat16)
    return serving_query, serving_key, serving_value, scale_query, scale_key, scale_value, serve_norm
```

```python
import functools

import jax
import jax.numpy as jnp
from jax import lax
from jax.experimental import pallas as pl
from jax.experimental.pallas import tpu as pltpu
from jax.sharding import PartitionSpec as P


mix_rate = 1.0
MIB = 1 << 20
f32, bf16 = jnp.float32, jnp.bfloat16
HBM, VMEM = pl.BlockSpec(memory_space=pltpu.HBM), pl.BlockSpec(memory_space=pltpu.VMEM)
DMA = pltpu.SemaphoreType.DMA
MESH = pl.DeviceIdType.MESH


def in_hbm(x):
    return pltpu.with_memory_space_constraint(x, pltpu.HBM)


def in_vmem(x):
    return pltpu.with_memory_space_constraint(x, pltpu.VMEM)


def product(low, rank, i, at, tile, high):
    return mix_rate * lax.dot_general(
        low[pl.ds(i * rank, rank), pl.ds(at, tile)], high[...],
        (((0,), (0,)), ((), ())), preferred_element_type=f32,
    )


def merge_kernel(n_shard, n_model, tile, first, rank, offsets, *refs):
    refs = list(refs)
    take = lambda n: [refs.pop(0) for _ in range(n)]
    trains, lows, highs = zip(*(take(3) for _ in range(3)))
    nt, ns = take(2)
    raws = take(1) if first < trains[0].shape[0] else []
    bufs, scales = take(3), take(3)
    norm, gq, far_low = take(3)
    wholes = take(3)
    low, gk, gv, raw_q, raw_k, raw_v = take(6)
    fars, products = take(3), take(3)
    norms, packs, sem_base, sem_small = take(4)
    send_norm, recv_norm, send_low, recv_low, send_far, recv_far, send_pack, recv_pack, ready, all_in = take(10)
    highs_in = (gq, gk, gv)
    rows = trains[0].shape[0]
    steps = rows // tile
    shard, model = lax.axis_index("shard"), lax.axis_index("model")
    group = n_shard * n_model
    place = shard * n_model + model
    lead = n_shard - 1
    leads, follows = shard == lead, shard != lead
    others = range(1, n_shard)

    def far(k):
        other = lax.rem(place + k, group)
        return {"shard": other // n_model, "model": lax.rem(other, n_model)}

    def near(d):
        return {"shard": lax.rem(shard + d, n_shard)}

    def remote(source, target, send, recv, device):
        return pltpu.make_async_remote_copy(
            src_ref=source, dst_ref=target, send_sem=send, recv_sem=recv,
            device_id=device, device_id_type=MESH,
        )

    def signal(semaphore, device):
        pl.semaphore_signal(semaphore, inc=1, device_id=device, device_id_type=MESH)

    barrier = pltpu.get_barrier_semaphore()
    for d in others:
        @pl.when(lax.rem(shard + d, n_shard) != lead)
        def _():
            signal(barrier, near(d))

    small = []
    for i in range(3):
        small.append(pltpu.make_async_copy(lows[i], low.at[pl.ds(i * rank, rank), :], sem_small.at[2 * i]))
        small.append(pltpu.make_async_copy(highs[i], highs_in[i], sem_small.at[2 * i + 1]))
    own_norm = [pltpu.make_async_copy(x, norms.at[place, j], sem_small.at[6 + j]) for j, x in enumerate((nt, ns))]
    for copy in own_norm + small:
        copy.start(priority=0)
    parts = [(0, first, raw_q)] + [(first, rows - first, raw) for raw in raws]

    def own_at(i, begin, count):
        if i:
            return (raw_k, raw_v)[i - 1].at[pl.ds(begin, count), :]
        start, _, ref = [p for p in parts if p[0] <= begin < p[0] + p[1]][0]
        return ref.at[pl.ds(begin - start, count), :]

    copies = [
        [
            pltpu.make_async_copy(trains[i].at[pl.ds(t * tile, tile), :], own_at(i, t * tile, tile), sem_base.at[t, i])
            for i in range(3)
        ]
        for t in range(steps)
    ]
    for t in range(steps):
        for copy in copies[t]:
            copy.start(priority=1)

    @pl.when(leads)
    def _():
        pl.semaphore_wait(ready, n_shard - 1)
        for m in range(1, n_model):
            signal(barrier, {"model": lax.rem(model + m, n_model)})

    @pl.when(follows)
    def _():
        pl.semaphore_wait(barrier, n_shard - 1)
        signal(ready, {"shard": lead})

    low_copies = [
        remote(lows[i], far_low.at[d - 1, pl.ds(i * rank, rank), :], send_low.at[d, i], recv_low.at[d, i], near(d))
        for d in others for i in range(3)
    ]
    far_copies = {}

    def pieces(i, count, size):
        for t in range(count // size):
            at = pl.ds(t * size, size)
            far_copies[i, t] = [
                remote(
                    trains[i].at[at, :], fars[i].at[d - 1, at, :],
                    send_far.at[i, t, d], recv_far.at[i, t, d], near(d),
                )
                for d in others
            ]

    sizes = (min(tile, first), rows // 2, rows // 4)
    counts = (first // sizes[0], 2, 4)
    for i in range(3):
        pieces(i, first if i == 0 else rows, sizes[i])

    def start(groups):
        for group_copies in groups:
            for copy in group_copies:
                copy.start()

    norm_copies = [
        remote(norms.at[place], norms.at[place], send_norm.at[k], recv_norm.at[k], far(k)) for k in range(1, group)
    ]

    def meet():
        @pl.when(leads)
        def _():
            pl.semaphore_wait(barrier, n_model - 1)
            for d in others:
                signal(all_in, near(d))

        @pl.when(follows)
        def _():
            pl.semaphore_wait(all_in, 1)

        start([norm_copies])

    keys, values = ([far_copies[i, t] for t in range(counts[i])] for i in (1, 2))
    early, late = model == 0, model == n_model - 1
    between = jnp.logical_not(jnp.logical_or(early, late))

    @pl.when(early)
    def _():
        start([low_copies] + keys + values + [far_copies[0, 0]])

    @pl.when(between)
    def _():
        start([low_copies] + keys + values[:1])

    for copy in own_norm:
        copy.wait()

    @pl.when(late)
    def _():
        meet()
        start([low_copies] + keys + values + [far_copies[0, 0]])

    for copy in small:
        copy.wait()
    for i in (1, 2):
        wholes[i][...] = product(low, rank, i, 0, rows, highs_in[i])
    wholes[0][...] = product(low, rank, 0, 0, rows, highs_in[0])

    @pl.when(between)
    def _():
        meet()
        start(values[1:] + [far_copies[0, 0]])

    tops = [jnp.zeros((8, h.shape[1]), f32) for h in highs]
    for t in range(steps):
        for copy in copies[t]:
            copy.wait()
        here = pl.ds(t * tile, tile)
        for i in range(3):
            whole = own_at(i, t * tile, tile)[...].astype(f32) + wholes[i][here, :]
            wholes[i][here, :] = whole
            tops[i] = jnp.maximum(tops[i], jnp.max(jnp.abs(whole).reshape(tile // 8, 8, whole.shape[1]), axis=0))
    packs[0] = jnp.zeros(packs.shape[1:], f32)
    for i in range(3):
        top = jnp.max(tops[i], axis=0, keepdims=True)
        for j in range(top.shape[1] // 128):
            packs[0, pl.ds(offsets[i] + j, 1), :] = top[:, j * 128:(j + 1) * 128]
    pack_copies = [remote(packs.at[0], packs.at[d], send_pack.at[d], recv_pack.at[d], near(d)) for d in others]
    start([pack_copies] + [far_copies[0, t] for t in range(1, counts[0])])
    for copy in low_copies:
        copy.wait()
    limits = (first, rows, rows)
    for d in range(n_shard - 1):
        for i in (1, 2, 0):
            products[i][d] = product(far_low.at[d], rank, i, 0, limits[i], highs_in[i])

    @pl.when(early)
    def _():
        meet()

    for copy in pack_copies:
        copy.wait()
    top = packs[0]
    for d in others:
        top = jnp.maximum(top, packs[d])
    inverse = []
    for i in range(3):
        block = top[offsets[i]:offsets[i] + scales[i].shape[1] // 128, :]
        line = jnp.concatenate([block[j:j + 1, :] for j in range(block.shape[0])], axis=1)
        scales[i][...] = line
        inverse.append(1.0 / line)
    for t in range(steps):
        at = pl.ds(t * tile, tile)
        for i in range(3):
            bufs[i][at, :] = (wholes[i][at, :] * inverse[i]).astype(bf16)
    for i in (1, 2, 0):
        for t in range(counts[i]):
            for copy in far_copies[i, t]:
                copy.wait()
            at = pl.ds(t * sizes[i], sizes[i])
            for d in range(n_shard - 1):
                whole = fars[i][d, at, :].astype(f32) + products[i][d, at, :]
                to = pl.ds(rows + d * limits[i] + t * sizes[i], sizes[i])
                bufs[i][to, :] = (whole * inverse[i]).astype(bf16)
    for copy in norm_copies:
        copy.wait()
    norm[...] = (norms[:, 0] + norms[:, 1]).reshape(norm.shape).astype(norm.dtype)


def write_kernel(rank, n_shard, first, rows, *refs):
    refs = list(refs)
    take = lambda n: [refs.pop(0) for _ in range(n)]
    bufs, scales = take(3), take(3)
    norm, gq, far_low = take(3)
    outs, lines = take(3), take(3)
    (norm_out,) = take(1)
    rest = take(1) if first < rows else []
    sems, small = take(2)
    shard = lax.axis_index("shard")
    made = []
    for i in (0, 1, 2):
        count = rows if i else first
        half = rows // 2
        for h in range(2):
            base = pl.multiple_of(shard * rows + h * half, half)
            made.append(pltpu.make_async_copy(
                bufs[i].at[pl.ds(h * half, half), :], outs[i].at[pl.ds(base, half), :], sems.at[i, 0, h]
            ))
        for d in range(1, n_shard):
            base = pl.multiple_of(lax.rem(shard + n_shard - d, n_shard) * rows, rows)
            made.append(pltpu.make_async_copy(
                bufs[i].at[pl.ds(rows + (d - 1) * count, count), :], outs[i].at[pl.ds(base, count), :], sems.at[i, d, 0]
            ))
    for i in range(3):
        made.append(pltpu.make_async_copy(scales[i], lines[i], small.at[i]))
    made.append(pltpu.make_async_copy(norm, norm_out, small.at[3]))
    for copy in made:
        copy.start()
    for r in rest:
        for d in range(n_shard - 1):
            r[d] = product(far_low.at[d], rank, 0, first, rows - first, gq)
    for copy in made:
        copy.wait()


def chunk_kernel(tile, n_shard, begin, rows, *refs):
    refs = list(refs)
    take = lambda n: [refs.pop(0) for _ in range(n)]
    _, scale, rest = take(3)
    raws = take(n_shard - 1)
    out, buf, sems = take(3)
    count = raws[0].shape[0]
    shard = lax.axis_index("shard")
    inverse = 1.0 / scale[...]
    made = []
    for d in range(1, n_shard):
        base = lax.rem(shard + n_shard - d, n_shard) * rows
        for t in range(count // tile):
            at = pl.ds(t * tile, tile)
            here = pl.ds((d - 1) * count + t * tile, tile)
            whole = raws[d - 1][at, :].astype(f32) + rest[d - 1, at, :]
            buf[here, :] = (whole * inverse).astype(bf16)
            there = pl.multiple_of(base + begin + t * tile, tile)
            made.append(pltpu.make_async_copy(buf.at[here, :], out.at[pl.ds(there, tile), :], sems.at[d, t]))
            made[-1].start()
    for copy in made:
        copy.wait()


def shift(x, axis, size, d):
    return lax.ppermute(x, axis, [(s, (s + d) % size) for s in range(size)])


def split(rows):
    tile = min(rows, 256)
    units = rows // tile
    return tile, tile * max(1, units // 2)


def local(n_shard, n_model, tq, lq, hq, tk, lk, hk, tv, lv, hv, nt, ns):
    rows, rank = tq.shape[0], hq.shape[0]
    widths = (tq.shape[1], tk.shape[1], tv.shape[1])
    tile, first = split(rows)
    steps = rows // tile
    group = n_shard * n_model
    full = n_shard * rows
    left = rows - first
    lanes = 128 if nt.shape[0] % 128 == 0 else nt.shape[0]
    piece = (nt.shape[0] // lanes, lanes)
    offsets, at = [], 0
    for w in widths:
        offsets.append(at)
        at += w // 128
    pack_rows = -(-at // 8) * 8
    others = range(1, n_shard)
    far = n_shard - 1
    limits = (first, rows, rows)
    cost = lambda size: pl.CostEstimate(flops=size, bytes_accessed=size, transcendentals=0)
    vm = pltpu.VMEM
    norm_shape = (group * piece[0], lanes)
    elements = sum(widths)
    scratch_bytes = 4 * rows * elements + 2 * rows * elements + 2 * full * elements + 4 * full * elements

    merged = pl.pallas_call(
        functools.partial(merge_kernel, n_shard, n_model, tile, first, rank, tuple(offsets)),
        out_shape=([vm((left, widths[0]), bf16)] if left else [])
        + [vm((rows + far * n, w), bf16) for n, w in zip(limits, widths)]
        + [vm((1, w), f32) for w in widths]
        + [vm(norm_shape, bf16), vm((rank, widths[0]), bf16), vm((far, 3 * rank, rows), bf16)],
        in_specs=[HBM] * 11,
        out_specs=[VMEM] * (9 + bool(left)),
        scratch_shapes=[vm((rows, w), f32) for w in widths]
        + [
            vm((3 * rank, rows), bf16), vm((rank, widths[1]), bf16), vm((rank, widths[2]), bf16),
            vm((first, widths[0]), bf16), vm((rows, widths[1]), bf16), vm((rows, widths[2]), bf16),
        ]
        + [vm((far, n, w), bf16) for n, w in zip(limits, widths)]
        + [vm((far, n, w), f32) for n, w in zip(limits, widths)]
        + [
            vm((group, 2) + piece, f32), vm((n_shard, pack_rows, 128), f32), DMA((steps, 3)), DMA((8,)),
            DMA((group,)), DMA((group,)), DMA((n_shard, 3)), DMA((n_shard, 3)),
            DMA((3, max(steps, 4), n_shard)), DMA((3, max(steps, 4), n_shard)), DMA((n_shard,)), DMA((n_shard,)),
            pltpu.SemaphoreType.REGULAR, pltpu.SemaphoreType.REGULAR,
        ],
        compiler_params=pltpu.CompilerParams(
            collective_id=0, has_side_effects=True, vmem_limit_bytes=min(40 * MIB, scratch_bytes + 4 * MIB),
        ),
        cost_estimate=cost(10**9),
        name="merge",
    )(*(in_hbm(x) for x in (tq, lq.T, hq, tk, lk.T, hk, tv, lv.T, hv, nt.reshape(piece), ns.reshape(piece))))
    query = [in_vmem(shift(merged[0], "shard", n_shard, d)) for d in others] if left else []
    merged = [in_vmem(x) for x in merged[bool(left):]]

    outs = pl.pallas_call(
        functools.partial(write_kernel, rank, n_shard, first, rows),
        out_shape=[jax.ShapeDtypeStruct((full, w), bf16) for w in widths]
        + [jax.ShapeDtypeStruct((1, w), f32) for w in widths]
        + [jax.ShapeDtypeStruct(norm_shape, bf16)]
        + ([vm((far, left, widths[0]), f32)] if left else []),
        in_specs=[VMEM] * 9,
        out_specs=[HBM] * 7 + [VMEM] * bool(left),
        scratch_shapes=[DMA((3, n_shard, 2)), DMA((4,))],
        compiler_params=pltpu.CompilerParams(vmem_limit_bytes=2 * MIB),
        cost_estimate=cost(10**9),
        name="write",
    )(*merged)
    oq, ok, ov, sq, sk, sv, norm = outs[:7]

    if left:
        step = min(tile, left)
        oq = pl.pallas_call(
            functools.partial(chunk_kernel, step, n_shard, first, rows),
            out_shape=jax.ShapeDtypeStruct((full, widths[0]), bf16),
            in_specs=[HBM] + [VMEM] * (2 + far),
            out_specs=HBM,
            scratch_shapes=[vm((far * left, widths[0]), bf16), DMA((n_shard, left // step))],
            input_output_aliases={0: 0},
            compiler_params=pltpu.CompilerParams(vmem_limit_bytes=2 * MIB + 2 * far * left * widths[0]),
            cost_estimate=cost(10**8),
            name="chunk",
        )(oq, merged[3], in_vmem(outs[7]), *query)
    return (oq, ok, ov, *(x.reshape(-1) for x in (sq, sk, sv, norm)))


def solution(mesh):
    in_specs = (
        P(("unit", "shard"), "model"),
        P(("unit", "shard"), None),
        P("unit", "model"),
        P(("unit", "shard"), "model"),
        P(("unit", "shard"), None),
        P("unit", "model"),
        P(("unit", "shard"), "model"),
        P(("unit", "shard"), None),
        P("unit", "model"),
        P(("unit", "shard", "model")),
        P(("unit", "shard", "model")),
    )
    out_specs = (
        P("unit", "model"),
        P("unit", "model"),
        P("unit", "model"),
        P(("unit", "model")),
        P(("unit", "model")),
        P(("unit", "model")),
        P("unit"),
    )
    n_shard, n_model = mesh.shape["shard"], mesh.shape["model"]

    def body(*args):
        return local(n_shard, n_model, *args)

    return jax.shard_map(body, mesh=mesh, in_specs=in_specs, out_specs=out_specs, check_vma=False)
```

```python
import functools

import jax
import jax.numpy as jnp
from jax import lax
from jax.experimental import pallas as pl
from jax.experimental.pallas import tpu as pltpu
from jax.sharding import PartitionSpec as P


mix_rate = 1.0
MIB = 1 << 20
f32, bf16 = jnp.float32, jnp.bfloat16
HBM, VMEM = pl.BlockSpec(memory_space=pltpu.HBM), pl.BlockSpec(memory_space=pltpu.VMEM)
DMA = pltpu.SemaphoreType.DMA
MESH = pl.DeviceIdType.MESH


def in_hbm(x):
    return pltpu.with_memory_space_constraint(x, pltpu.HBM)


def in_vmem(x):
    return pltpu.with_memory_space_constraint(x, pltpu.VMEM)


def product(low, rank, i, at, tile, high):
    return mix_rate * lax.dot_general(
        low[pl.ds(i * rank, rank), pl.ds(at, tile)], high[...],
        (((0,), (0,)), ((), ())), preferred_element_type=f32,
    )


def merge_kernel(n_shard, n_model, tile, first, rank, offsets, *refs):
    refs = list(refs)
    take = lambda n: [refs.pop(0) for _ in range(n)]
    trains, lows, highs = zip(*(take(3) for _ in range(3)))
    nt, ns = take(2)
    raws = take(1) if first < trains[0].shape[0] else []
    (scaled,) = take(1)
    wholes, scales = take(2), take(3)
    (norm,) = take(1)
    fars, products = take(3), take(3)
    wholes = take(1) + wholes
    low, far_low, gq, gk, gv, raw_q, raw_k, raw_v = take(8)
    norms, sums, packs, sem_base, sem_small = take(5)
    send_norm, recv_norm, send_off, recv_off, send_low, recv_low = take(6)
    send_far, recv_far, send_pack, recv_pack, ready = take(5)
    highs_in = (gq, gk, gv)
    rows = trains[0].shape[0]
    steps = rows // tile
    shard, model = lax.axis_index("shard"), lax.axis_index("model")
    lead = n_shard - 1
    leads, follows = shard == lead, shard != lead
    others = range(1, n_shard)

    def near(d):
        return {"shard": lax.rem(shard + d, n_shard)}

    def remote(source, target, send, recv, device):
        return pltpu.make_async_remote_copy(
            src_ref=source, dst_ref=target, send_sem=send, recv_sem=recv,
            device_id=device, device_id_type=MESH,
        )

    def signal(semaphore, device):
        pl.semaphore_signal(semaphore, inc=1, device_id=device, device_id_type=MESH)

    barrier = pltpu.get_barrier_semaphore()
    for d in others:
        @pl.when(lax.rem(shard + d, n_shard) != lead)
        def _():
            signal(barrier, near(d))

    small = []
    for i in range(3):
        small.append(pltpu.make_async_copy(lows[i], low.at[pl.ds(i * rank, rank), :], sem_small.at[2 * i]))
        small.append(pltpu.make_async_copy(highs[i], highs_in[i], sem_small.at[2 * i + 1]))
    own_norm = [pltpu.make_async_copy(x, norms.at[model, shard, j], sem_small.at[6 + j]) for j, x in enumerate((nt, ns))]
    for copy in own_norm + small:
        copy.start(priority=0)
    parts = [(0, rows, raw_q)]

    def own_at(i, begin, count):
        if i:
            return (raw_k, raw_v)[i - 1].at[pl.ds(begin, count), :]
        start, _, ref = [p for p in parts if p[0] <= begin < p[0] + p[1]][0]
        return ref.at[pl.ds(begin - start, count), :]

    copies = [
        [
            pltpu.make_async_copy(trains[i].at[pl.ds(t * tile, tile), :], own_at(i, t * tile, tile), sem_base.at[t, i])
            for i in range(3)
        ]
        for t in range(steps)
    ]
    copies[-1] += [
        pltpu.make_async_copy(trains[0].at[pl.ds(first, rows - first), :], raw, sem_base.at[steps, 0]) for raw in raws
    ]

    @pl.when(leads)
    def _():
        pl.semaphore_wait(ready, n_shard - 1)
        for m in range(1, n_model):
            signal(barrier, {"model": lax.rem(model + m, n_model)})

    @pl.when(follows)
    def _():
        pl.semaphore_wait(barrier, n_shard - 1)
        signal(ready, {"shard": lead})

    low_copies = [
        remote(lows[i], far_low.at[d - 1, pl.ds(i * rank, rank), :], send_low.at[d, i], recv_low.at[d, i], near(d))
        for d in others for i in range(3)
    ]
    far_copies = {}

    def pieces(i, count, size):
        for t in range(count // size):
            at = pl.ds(t * size, size)
            source = raw_q if i == 0 and t > 1 else trains[i]
            far_copies[i, t] = [
                remote(
                    source.at[at, :], fars[i].at[d - 1, at, :],
                    send_far.at[i, t, d], recv_far.at[i, t, d], near(d),
                )
                for d in others
            ]

    sizes = (first // 7, rows // 2, rows // 4)
    counts = (7, 2, 4)
    for i in range(3):
        pieces(i, first if i == 0 else rows, sizes[i])

    def start(groups):
        for group_copies in groups:
            for copy in group_copies:
                copy.start()

    norm_copies = [
        remote(x, norms.at[model, shard, j], send_norm.at[d, j], recv_norm.at[d, j], near(d))
        for d in others for j, x in enumerate((nt, ns))
    ]

    def column_copy(k, s, source):
        return remote(
            norms.at[source], norms.at[source], send_off.at[k, s], recv_off.at[k],
            {"shard": s, "model": lax.rem(model + k, n_model)},
        )

    off_copies = [column_copy(k, s, model) for k in range(1, n_model) for s in range(n_shard)]

    def meet(role):
        @pl.when(jnp.logical_and(leads, role))
        def _():
            pl.semaphore_wait(barrier, n_model - 1)
            for copy in norm_copies:
                copy.wait_recv()
            for copy in off_copies:
                copy.start()

    keys, values = ([far_copies[i, t] for t in range(counts[i])] for i in (1, 2))
    early, late = model == 0, model == n_model - 1
    start([norm_copies, low_copies] + keys)
    for copies_at in copies:
        for copy in copies_at:
            copy.start(priority=1)
    start(values + [far_copies[0, u] for u in range(2)])
    for copy in own_norm:
        copy.wait()
    for copy in small:
        copy.wait()
    meet(late)
    for i in (1, 2):
        wholes[i][...] = product(low, rank, i, 0, rows, highs_in[i])
    meet(jnp.logical_not(jnp.logical_or(early, late)))
    wholes[0][...] = product(low, rank, 0, 0, rows, highs_in[0])

    tops = [jnp.zeros((8, h.shape[1]), f32) for h in highs]
    for t in range(steps):
        for copy in copies[t]:
            copy.wait()
        here = pl.ds(t * tile, tile)
        for i in range(3):
            whole = own_at(i, t * tile, tile)[...].astype(f32) + wholes[i][here, :]
            wholes[i][here, :] = whole
            tops[i] = jnp.maximum(tops[i], jnp.max(jnp.abs(whole).reshape(tile // 8, 8, whole.shape[1]), axis=0))
        if t == max(0, steps // 2 - 1):
            start([far_copies[0, u] for u in range(2, 4)])
    packs[0] = jnp.zeros(packs.shape[1:], f32)
    for i in range(3):
        top = jnp.max(tops[i], axis=0, keepdims=True)
        for j in range(top.shape[1] // 128):
            packs[0, pl.ds(offsets[i] + j, 1), :] = top[:, j * 128:(j + 1) * 128]
    pack_copies = [remote(packs.at[0], packs.at[d], send_pack.at[d], recv_pack.at[d], near(d)) for d in others]
    start([pack_copies] + [far_copies[0, t] for t in range(4, counts[0])])
    for copy in low_copies:
        copy.wait()
    for d in range(n_shard - 1):
        for i in (1, 2, 0):
            products[i][d] = product(far_low.at[d], rank, i, 0, rows, highs_in[i])

    meet(early)

    for copy in pack_copies:
        copy.wait()
    top = packs[0]
    for d in others:
        top = jnp.maximum(top, packs[d])
    for i in range(3):
        block = top[offsets[i]:offsets[i] + scales[i].shape[1] // 128, :]
        line = jnp.concatenate([block[j:j + 1, :] for j in range(block.shape[0])], axis=1)
        scales[i][...] = line
        if i == 0:
            scaled[...] = (wholes[0][...] * (1.0 / line)).astype(bf16)
    for i in (1, 2, 0):
        for t in range(counts[i]):
            for copy in far_copies[i, t]:
                copy.wait()

    @pl.when(leads)
    def _():
        for copy in norm_copies:
            copy.wait_send()
        for copy in off_copies:
            copy.wait_send()

    @pl.when(follows)
    def _():
        for copy in norm_copies:
            copy.wait()

    for k in range(1, n_model):
        column_copy(k, 0, lax.rem(model + n_model - k, n_model)).wait_recv()
    for s in range(n_shard):
        for m in range(n_model):
            sums[s, m] = norms[m, s, 0] + norms[m, s, 1]
    norm[...] = sums[...].reshape(norm.shape).astype(norm.dtype)


def write_kernel(n_shard, first, rows, *refs):
    refs = list(refs)
    take = lambda n: [refs.pop(0) for _ in range(n)]
    (scaled,) = take(1)
    wholes, scales = take(2), take(3)
    (norm,) = take(1)
    fars, products = take(3), take(3)
    outs, lines = take(3), take(3)
    (norm_out,) = take(1)
    bufs = take(3)
    sems, small = take(2)
    shard = lax.axis_index("shard")
    limits = (first, rows, rows)
    made = [pltpu.make_async_copy(scales[i], lines[i], small.at[i]) for i in range(3)]
    made.append(pltpu.make_async_copy(norm, norm_out, small.at[3]))
    inverse = [1.0 / scales[i][...] for i in range(3)]

    def put(i, d, t, size, whole):
        here = pl.ds(((rows if i else 0) + (d - 1) * limits[i] if d else 0) + t * size, size)
        bufs[i][here, :] = (whole * inverse[i]).astype(bf16)
        there = pl.multiple_of(lax.rem(shard + n_shard - d, n_shard) * rows + t * size, size)
        made.append(pltpu.make_async_copy(bufs[i].at[here, :], outs[i].at[pl.ds(there, size), :], sems.at[i, d, t]))
        made[-1].start()

    for t in range(2):
        size = rows // 2
        there = pl.multiple_of(shard * rows + t * size, size)
        made.append(pltpu.make_async_copy(
            scaled.at[pl.ds(t * size, size), :], outs[0].at[pl.ds(there, size), :], sems.at[0, 0, t]
        ))
        made[-1].start()
    for copy in made[:4]:
        copy.start()
    for i in (1, 2):
        for t in range(2):
            size = rows // 2
            put(i, 0, t, size, wholes[i - 1][pl.ds(t * size, size), :])
    for d in range(1, n_shard):
        for i in (1, 2, 0):
            size = first // 7 if i == 0 else rows // 2
            for t in range(limits[i] // size):
                at = pl.ds(t * size, size)
                put(i, d, t, size, fars[i][d - 1, at, :].astype(f32) + products[i][d - 1, at, :])
    for copy in made:
        copy.wait()


def chunk_kernel(tile, n_shard, begin, rows, *refs):
    refs = list(refs)
    take = lambda n: [refs.pop(0) for _ in range(n)]
    _, scale, rest = take(3)
    raws = take(n_shard - 1)
    out, buf, sems = take(3)
    count = raws[0].shape[0]
    shard = lax.axis_index("shard")
    inverse = 1.0 / scale[...]
    made = []
    for d in range(1, n_shard):
        base = lax.rem(shard + n_shard - d, n_shard) * rows
        for t in range(count // tile):
            at = pl.ds(t * tile, tile)
            here = pl.ds((d - 1) * count + t * tile, tile)
            whole = raws[d - 1][at, :].astype(f32) + rest[d - 1, pl.ds(begin + t * tile, tile), :]
            buf[here, :] = (whole * inverse).astype(bf16)
            there = pl.multiple_of(base + begin + t * tile, tile)
            made.append(pltpu.make_async_copy(buf.at[here, :], out.at[pl.ds(there, tile), :], sems.at[d, t]))
            made[-1].start()
    for copy in made:
        copy.wait()


def shift(x, axis, size, d):
    return lax.ppermute(x, axis, [(s, (s + d) % size) for s in range(size)])


def split(rows):
    tile = min(rows, 256)
    return tile, 7 * rows // 16


def local(n_shard, n_model, tq, lq, hq, tk, lk, hk, tv, lv, hv, nt, ns):
    rows, rank = tq.shape[0], hq.shape[0]
    widths = (tq.shape[1], tk.shape[1], tv.shape[1])
    tile, first = split(rows)
    steps = rows // tile
    group = n_shard * n_model
    full = n_shard * rows
    left = rows - first
    lanes = 128 if nt.shape[0] % 128 == 0 else nt.shape[0]
    piece = (nt.shape[0] // lanes, lanes)
    offsets, at = [], 0
    for w in widths:
        offsets.append(at)
        at += w // 128
    pack_rows = -(-at // 8) * 8
    others = range(1, n_shard)
    far = n_shard - 1
    limits = (first, rows, rows)
    cost = lambda size: pl.CostEstimate(flops=size, bytes_accessed=size, transcendentals=0)
    vm = pltpu.VMEM
    norm_shape = (group * piece[0], lanes)
    elements = sum(widths)
    scratch_bytes = 4 * rows * widths[0] + 2 * rows * elements + 12 * full * rank

    merged = pl.pallas_call(
        functools.partial(merge_kernel, n_shard, n_model, tile, first, rank, tuple(offsets)),
        out_shape=([vm((left, widths[0]), bf16)] if left else [])
        + [vm((rows, widths[0]), bf16)]
        + [vm((rows, w), f32) for w in widths[1:]]
        + [vm((1, w), f32) for w in widths]
        + [vm(norm_shape, bf16)]
        + [vm((far, n, w), bf16) for n, w in zip(limits, widths)]
        + [vm((far, rows, w), f32) for w in widths],
        in_specs=[HBM] * 11,
        out_specs=[VMEM] * (13 + bool(left)),
        scratch_shapes=[vm((rows, widths[0]), f32), vm((3 * rank, rows), bf16), vm((far, 3 * rank, rows), bf16)]
        + [vm((rank, w), bf16) for w in widths]
        + [vm((rows, widths[0]), bf16), vm((rows, widths[1]), bf16), vm((rows, widths[2]), bf16)]
        + [
            vm((n_model, n_shard, 2) + piece, f32), vm((n_shard, n_model) + piece, f32),
            vm((n_shard, pack_rows, 128), f32), DMA((steps + 1, 3)), DMA((8,)),
            DMA((n_shard, 2)), DMA((n_shard, 2)), DMA((n_model, n_shard)), DMA((n_model,)),
            DMA((n_shard, 3)), DMA((n_shard, 3)),
            DMA((3, 7, n_shard)), DMA((3, 7, n_shard)), DMA((n_shard,)), DMA((n_shard,)),
            pltpu.SemaphoreType.REGULAR,
        ],
        compiler_params=pltpu.CompilerParams(
            collective_id=0, has_side_effects=True, vmem_limit_bytes=scratch_bytes + 4 * MIB,
        ),
        cost_estimate=cost(10**9),
        name="merge",
    )(*(in_hbm(x) for x in (tq, lq.T, hq, tk, lk.T, hk, tv, lv.T, hv, nt.reshape(piece), ns.reshape(piece))))
    query = [in_vmem(shift(merged[0], "shard", n_shard, d)) for d in others] if left else []
    merged = [in_vmem(x) for x in merged[bool(left):]]

    outs = pl.pallas_call(
        functools.partial(write_kernel, n_shard, first, rows),
        out_shape=[jax.ShapeDtypeStruct((full, w), bf16) for w in widths]
        + [jax.ShapeDtypeStruct((1, w), f32) for w in widths]
        + [jax.ShapeDtypeStruct(norm_shape, bf16)],
        in_specs=[VMEM] * 13,
        out_specs=[HBM] * 7,
        scratch_shapes=[vm(((rows if i else 0) + far * n, w), bf16) for i, (n, w) in enumerate(zip(limits, widths))]
        + [DMA((3, n_shard, 7)), DMA((4,))],
        compiler_params=pltpu.CompilerParams(vmem_limit_bytes=3 * MIB + 2 * full * elements),
        cost_estimate=cost(10**9),
        name="write",
    )(*merged)
    oq, ok, ov, sq, sk, sv, norm = outs

    if left:
        step = left // 9
        oq = pl.pallas_call(
            functools.partial(chunk_kernel, step, n_shard, first, rows),
            out_shape=jax.ShapeDtypeStruct((full, widths[0]), bf16),
            in_specs=[HBM] + [VMEM] * (2 + far),
            out_specs=HBM,
            scratch_shapes=[vm((far * left, widths[0]), bf16), DMA((n_shard, left // step))],
            input_output_aliases={0: 0},
            compiler_params=pltpu.CompilerParams(vmem_limit_bytes=2 * MIB + 2 * far * left * widths[0]),
            cost_estimate=cost(10**8),
            name="chunk",
        )(oq, merged[3], merged[10], *query)
    return (oq, ok, ov, *(x.reshape(-1) for x in (sq, sk, sv, norm)))


def solution(mesh):
    in_specs = (
        P(("unit", "shard"), "model"),
        P(("unit", "shard"), None),
        P("unit", "model"),
        P(("unit", "shard"), "model"),
        P(("unit", "shard"), None),
        P("unit", "model"),
        P(("unit", "shard"), "model"),
        P(("unit", "shard"), None),
        P("unit", "model"),
        P(("unit", "shard", "model")),
        P(("unit", "shard", "model")),
    )
    out_specs = (
        P("unit", "model"),
        P("unit", "model"),
        P("unit", "model"),
        P(("unit", "model")),
        P(("unit", "model")),
        P(("unit", "model")),
        P("unit"),
    )
    n_shard, n_model = mesh.shape["shard"], mesh.shape["model"]

    def body(*args):
        return local(n_shard, n_model, *args)

    return jax.shard_map(body, mesh=mesh, in_specs=in_specs, out_specs=out_specs, check_vma=False)
```
